32 devices in a mesh: rep: 2 (over z, core), dp: 16 (over x, y).
Axes of the slice: x: 4, y: 4, z: 1, core: 2. Of those that a mesh axis runs over, the one named last changes fastest.
The devices are a block of a 4x4x8 slice.
Arguments:
- a: bfloat16 [32, 4, 4096, 896], P(('rep', 'dp')), parts along dimension 0
- g: bfloat16 [32, 4, 4096, 2304], P(('rep', 'dp')), parts along dimension 0
Outputs:
- output: bfloat16 [8, 896, 2304], P('rep'), parts along dimension 0
There are 2 independent parts. The reference program is written for one: setup_inputs(seed, part) draws one part's arguments, and reference() takes and returns one part's arrays. A program takes and returns all parts, laid end to end along the dimension named above; each array names one.
All inputs are finite; a program needn't handle non-finite values.
Results may differ from the reference program's by a relative error of at most 0.012.
Values are sent between devices in bfloat16 or wider.
A program may use at most 768 MiB of HBM per device.

```python
import jax
import jax.numpy as jnp
from jax import lax

DEVICES = 16
MATRICES = 4
TOKENS = 4096
D = 896
FF = 2304


def setup_inputs(seed: int = 0, part: int = 0) -> dict:
    ka, kg, ks = (jax.random.fold_in(k, part) for k in jax.random.split(jax.random.key(seed), 3))
    size = 2.0 ** jax.random.uniform(ks, (DEVICES, MATRICES, 1, 1), jnp.float32, -1.0, 1.0)
    a = jax.random.normal(ka, (DEVICES, MATRICES, TOKENS, D), jnp.float32)
    g = size * jax.random.normal(kg, (DEVICES, MATRICES, TOKENS, FF), jnp.float32) * (DEVICES * TOKENS) ** -0.5
    return {"a": a.astype(jnp.bfloat16), "g": g.astype(jnp.bfloat16)}


def reference(a, g):
    def take(so_far, one):
        return so_far + jnp.einsum("ntd,ntf->ndf", *one, preferred_element_type=jnp.float32), None

    return lax.scan(take, jnp.zeros((MATRICES, D, FF), jnp.float32), (a, g))[0].astype(jnp.bfloat16)
```

```python
import functools
import math

import jax
import jax.numpy as jnp
from jax import lax
from jax.experimental import pallas as pl
from jax.experimental.pallas import tpu as pltpu
from jax.sharding import PartitionSpec as P

MESH = pl.DeviceIdType.MESH
F32, BF16 = jnp.float32, jnp.bfloat16

WIDTH = 256
LAG = 2
STAGES = 10
LANDING = 4 * LAG + 4
LEAVING = 2 * LAG + 2
TURN = 512


def kernel(side, a_hbm, g_hbm, out, raw, turned, g_buf, acc, half, far_out, near_out, far_in, near_in, raw_sem, g_sem, send, recv):
    matrices, tokens, d = a_hbm.shape
    per_matrix = g_hbm.shape[2] // WIDTH
    pieces = matrices * per_matrix
    quarter = d // side
    part = quarter // side
    rep, me = lax.axis_index("rep"), lax.axis_index("dp")

    def step_from(axis, delta):
        stride = side * (1 - axis) + axis
        at = (me // stride) % side
        return me + ((at + delta + side) % side - at) * stride

    barrier = pltpu.get_barrier_semaphore()
    for axis in (0, 1):
        for delta in (1, -1):
            pl.semaphore_signal(barrier, inc=1, device_id=(rep, step_from(axis, delta)), device_id_type=MESH)

    def load_a(n):
        return pltpu.make_async_copy(a_hbm.at[n], raw, raw_sem)

    def load_g(k):
        columns = pl.ds(pl.multiple_of((k % per_matrix) * WIDTH, WIDTH), WIDTH)
        return pltpu.make_async_copy(g_hbm.at[k // per_matrix, :, columns], g_buf.at[k % 2], g_sem.at[k % 2])

    load_a(0).start()
    load_g(0).start()
    pl.semaphore_wait(barrier, 4)

    class Piece:
        def __init__(self, k):
            self.k = k
            self.axis = k % 2
            self.way = 1 - 2 * ((k // 2 + rep) % 2)
            stride = side * (1 - self.axis) + self.axis
            self.at = ((me // stride) % side, (me // (side + 1 - stride)) % side)
            self.land, self.leave = k % LANDING, k % LEAVING

        def rows(self, phase, delta):
            size = (quarter, part)[phase]
            owner = (self.at[phase] + delta * self.way + 2 * side) % side
            return pl.ds(pl.multiple_of(owner * size, size), size)

        def own(self, delta):
            owner = (self.at[1] + delta * self.way + 2 * side) % side
            return pl.ds(pl.multiple_of(self.at[0] * quarter + owner * part, part), part)

        def copy(self, src, dst, phase, message):
            second = 1 if phase in (1, 2) else 0
            axis = self.axis * (1 - second) + (1 - self.axis) * second
            delta = self.way if message != 1 else -self.way
            return pltpu.make_async_remote_copy(
                src_ref=src,
                dst_ref=dst,
                send_sem=send.at[phase, message, self.leave],
                recv_sem=recv.at[phase, message, self.land],
                device_id=(rep, step_from(axis, delta)),
                device_id_type=MESH,
            )

        def reduce_copy(self, phase, message):
            leaving, landing = ((far_out, far_in), (near_out, near_in))[phase]
            return self.copy(leaving.at[self.leave, message], landing.at[self.land, message], phase, message)

        def landed(self, phase, message):
            return ((far_in, near_in)[phase])[self.land, message].astype(F32)

        def gather_copy(self, phase, message, rows):
            where = out.at[self.k, rows, :]
            return self.copy(where, where, phase, message)

        def gather_rows(self, phase, message):
            delta = 0 if message != 2 else -1
            return self.own(delta) if phase == 2 else self.rows(0, delta)

        def gather(self, phase, message):
            return self.gather_copy(phase, message, self.gather_rows(phase, message))

    def stage0(k):
        n, j = k // per_matrix, k % per_matrix

        @pl.when(j == 0)
        def _():
            load_a(n).wait()

            @pl.loop(0, tokens // TURN)
            def _(t):
                at = pl.multiple_of(t * TURN, TURN)
                turned[:, pl.ds(at, TURN)] = raw[pl.ds(at, TURN), :].T

            @pl.when(n + 1 < matrices)
            def _():
                load_a(n + 1).start()

        load_g(k).wait()

        @pl.when(k + 1 < pieces)
        def _():
            load_g(k + 1).start()

        p = Piece(k)
        slot = k % LEAVING

        @pl.loop(0, side)
        def _(r):
            rows = pl.ds(pl.multiple_of(r * quarter, quarter), quarter)
            acc[slot, rows, :] = jnp.dot(turned[rows, :], g_buf[k % 2], preferred_element_type=F32)

        far_out[p.leave, 0] = acc[slot, p.rows(0, 2), :].astype(BF16)
        far_out[p.leave, 1] = acc[slot, p.rows(0, -1), :].astype(BF16)
        p.reduce_copy(0, 0).start()
        p.reduce_copy(0, 1).start()

    def stage1(k):
        p = Piece(k)
        p.reduce_copy(0, 0).wait_recv()
        far_out[p.leave, 2] = (acc[k % LEAVING, p.rows(0, 1), :] + p.landed(0, 0)).astype(BF16)
        p.reduce_copy(0, 2).start()

    def stage2(k):
        p = Piece(k)
        p.reduce_copy(0, 1).wait_recv()
        p.reduce_copy(0, 2).wait_recv()
        slot = k % LEAVING
        half[slot] = acc[slot, p.rows(0, 0), :] + p.landed(0, 1) + p.landed(0, 2)
        near_out[p.leave, 0] = half[slot, p.rows(1, 2), :].astype(BF16)
        near_out[p.leave, 1] = half[slot, p.rows(1, -1), :].astype(BF16)
        p.reduce_copy(0, 0).wait_send()
        p.reduce_copy(0, 1).wait_send()
        p.reduce_copy(1, 0).start()
        p.reduce_copy(1, 1).start()

    def stage3(k):
        p = Piece(k)
        p.reduce_copy(1, 0).wait_recv()
        near_out[p.leave, 2] = (half[k % LEAVING, p.rows(1, 1), :] + p.landed(1, 0)).astype(BF16)
        p.reduce_copy(0, 2).wait_send()
        p.reduce_copy(1, 2).start()

    def stage4(k):
        p = Piece(k)
        p.reduce_copy(1, 1).wait_recv()
        p.reduce_copy(1, 2).wait_recv()
        out[k, p.own(0), :] = (half[k % LEAVING, p.rows(1, 0), :] + p.landed(1, 1) + p.landed(1, 2)).astype(BF16)
        p.reduce_copy(1, 0).wait_send()
        p.reduce_copy(1, 1).wait_send()
        p.gather(2, 0).start()
        p.gather(2, 1).start()

    def stage5(k):
        p = Piece(k)
        p.gather(2, 0).wait_recv()
        p.reduce_copy(1, 2).wait_send()
        p.gather(2, 2).start()

    def stage6(k):
        p = Piece(k)
        p.gather(2, 1).wait_recv()
        p.gather(2, 2).wait_recv()
        p.gather(2, 0).wait_send()
        p.gather(2, 1).wait_send()
        p.gather(3, 0).start()
        p.gather(3, 1).start()

    def stage7(k):
        p = Piece(k)
        p.gather(3, 0).wait_recv()
        p.gather(2, 2).wait_send()
        p.gather(3, 2).start()

    def stage8(k):
        p = Piece(k)
        p.gather(3, 1).wait_recv()
        p.gather(3, 2).wait_recv()
        p.gather(3, 0).wait_send()
        p.gather(3, 1).wait_send()

    def stage9(k):
        Piece(k).gather(3, 2).wait_send()

    stages = (stage0, stage1, stage2, stage3, stage4, stage5, stage6, stage7, stage8, stage9)
    assert len(stages) == STAGES

    @pl.loop(0, pieces + (STAGES - 1) * LAG)
    def _(i):
        for s in reversed(range(STAGES)):
            k = i - s * LAG

            @pl.when((k >= 0) & (k < pieces))
            def _(s=s, k=k):
                stages[s](k)


def place(held, out, sem):
    matrices, per_matrix = out.shape[0], out.shape[2] // WIDTH

    def move(k):
        columns = pl.ds(pl.multiple_of((k % per_matrix) * WIDTH, WIDTH), WIDTH)
        return pltpu.make_async_copy(held.at[k], out.at[k // per_matrix, :, columns], sem.at[k])

    for k in range(matrices * per_matrix):
        move(k).start()
    for k in range(matrices * per_matrix):
        move(k).wait()


def solution(mesh):
    side = math.isqrt(mesh.shape["dp"])

    def local(a, g):
        a, g = a[0], g[0]
        matrices, tokens, d = a.shape
        ff = g.shape[2]
        pieces = matrices * (ff // WIDTH)
        quarter = d // side
        part = quarter // side
        held = pl.pallas_call(
            functools.partial(kernel, side),
            out_shape=pltpu.VMEM((pieces, d, WIDTH), BF16),
            in_specs=[pl.BlockSpec(memory_space=pltpu.HBM)] * 2,
            out_specs=pl.BlockSpec(memory_space=pltpu.VMEM),
            scratch_shapes=[
                pltpu.VMEM((tokens, d), BF16),
                pltpu.VMEM((d, tokens), BF16),
                pltpu.VMEM((2, tokens, WIDTH), BF16),
                pltpu.VMEM((LEAVING, d, WIDTH), F32),
                pltpu.VMEM((LEAVING, quarter, WIDTH), F32),
                pltpu.VMEM((LEAVING, 3, quarter, WIDTH), BF16),
                pltpu.VMEM((LEAVING, 3, part, WIDTH), BF16),
                pltpu.VMEM((LANDING, 3, quarter, WIDTH), BF16),
                pltpu.VMEM((LANDING, 3, part, WIDTH), BF16),
                pltpu.SemaphoreType.DMA,
                pltpu.SemaphoreType.DMA((2,)),
                pltpu.SemaphoreType.DMA((4, 3, LEAVING)),
                pltpu.SemaphoreType.DMA((4, 3, LANDING)),
            ],
            compiler_params=pltpu.CompilerParams(
                collective_id=0, has_side_effects=True, vmem_limit_bytes=44 * 2**20
            ),
            cost_estimate=pl.CostEstimate(
                flops=2 * matrices * tokens * d * ff,
                bytes_accessed=2 * matrices * tokens * (d + ff),
                transcendentals=0,
            ),
            name="sum_over_group",
        )(a, g)
        return pl.pallas_call(
            place,
            out_shape=jax.ShapeDtypeStruct((matrices, d, ff), BF16),
            in_specs=[pl.BlockSpec(memory_space=pltpu.VMEM)],
            out_specs=pl.BlockSpec(memory_space=pltpu.HBM),
            scratch_shapes=[pltpu.SemaphoreType.DMA((pieces,))],
            compiler_params=pltpu.CompilerParams(vmem_limit_bytes=2**20),
            name="place",
        )(held)

    return jax.shard_map(
        local,
        mesh=mesh,
        in_specs=(P(("rep", "dp")), P(("rep", "dp"))),
        out_specs=P("rep"),
        check_vma=False,
    )
```

```python
import functools
import math

import jax
import jax.numpy as jnp
from jax import lax
from jax.experimental import pallas as pl
from jax.experimental.pallas import tpu as pltpu
from jax.sharding import PartitionSpec as P

MESH = pl.DeviceIdType.MESH
F32, BF16 = jnp.float32, jnp.bfloat16

WIDTH = 256
LAGS = (0, 3, 6, 9, 12, 15, 18, 21, 24, 27)
LEAVING = max(later - sooner for sooner, later in zip(LAGS, LAGS[2:]))
LANDING = 2 * LEAVING + 4
TURN = 512
RAW = 4
AHEAD = 2


def kernel(side, a_hbm, g_hbm, out, raw, turned_even, turned_odd, g_buf, acc, half, far_out, near_out, far_in, near_in, raw_sem, g_sem, send, recv):
    matrices, tokens, d = a_hbm.shape
    per_matrix = g_hbm.shape[2] // WIDTH
    pieces = matrices * per_matrix
    quarter = d // side
    part = quarter // side
    rep, me = lax.axis_index("rep"), lax.axis_index("dp")

    def step_from(axis, delta):
        stride = side * (1 - axis) + axis
        at = (me // stride) % side
        return me + ((at + delta + side) % side - at) * stride

    barrier = pltpu.get_barrier_semaphore()
    for axis in (0, 1):
        for delta in (1, -1):
            pl.semaphore_signal(barrier, inc=1, device_id=(rep, step_from(axis, delta)), device_id_type=MESH)

    blocks = tokens // TURN

    def load_a(q):
        at = pl.ds(pl.multiple_of((q % blocks) * TURN, TURN), TURN)
        return pltpu.make_async_copy(a_hbm.at[q // blocks, at, :], raw.at[q % RAW], raw_sem.at[q % RAW])

    def load_g(k):
        columns = pl.ds(pl.multiple_of((k % per_matrix) * WIDTH, WIDTH), WIDTH)
        slot = k % (AHEAD + 1)
        return pltpu.make_async_copy(g_hbm.at[k // per_matrix, :, columns], g_buf.at[slot], g_sem.at[slot])

    def turn(q, turned):
        at = pl.ds(pl.multiple_of((q % blocks) * TURN, TURN), TURN)
        turned[:, at] = raw[q % RAW].T

    for q in range(RAW):
        load_a(q).start()
    for k in range(AHEAD):
        load_g(k).start()

    @pl.loop(0, blocks)
    def _(q):
        load_a(q).wait()

        @pl.when(q > 0)
        def _():
            load_a(q - 1 + RAW).start()

        turn(q, turned_even)

    pl.semaphore_wait(barrier, 4)

    class Piece:
        def __init__(self, k):
            self.k = k
            self.axis = k % 2
            self.way = 1 - 2 * ((k // 2 + rep) % 2)
            stride = side * (1 - self.axis) + self.axis
            self.at = ((me // stride) % side, (me // (side + 1 - stride)) % side)
            self.land, self.leave = k % LANDING, k % LEAVING

        def rows(self, phase, delta):
            size = (quarter, part)[phase]
            owner = (self.at[phase] + delta * self.way + 2 * side) % side
            return pl.ds(pl.multiple_of(owner * size, size), size)

        def own(self, delta):
            owner = (self.at[1] + delta * self.way + 2 * side) % side
            return pl.ds(pl.multiple_of(self.at[0] * quarter + owner * part, part), part)

        def copy(self, src, dst, phase, message):
            second = 1 if phase in (1, 2) else 0
            axis = self.axis * (1 - second) + (1 - self.axis) * second
            delta = self.way if message != 1 else -self.way
            return pltpu.make_async_remote_copy(
                src_ref=src,
                dst_ref=dst,
                send_sem=send.at[phase, message, self.leave],
                recv_sem=recv.at[phase, message, self.land],
                device_id=(rep, step_from(axis, delta)),
                device_id_type=MESH,
            )

        def reduce_copy(self, phase, message):
            leaving, landing = ((far_out, far_in), (near_out, near_in))[phase]
            return self.copy(leaving.at[self.leave, message], landing.at[self.land, message], phase, message)

        def landed(self, phase, message):
            return ((far_in, near_in)[phase])[self.land, message].astype(F32)

        def gather_copy(self, phase, message, rows):
            where = out.at[self.k, rows, :]
            return self.copy(where, where, phase, message)

        def gather_rows(self, phase, message):
            delta = 0 if message != 2 else -1
            return self.own(delta) if phase == 2 else self.rows(0, delta)

        def gather(self, phase, message):
            return self.gather_copy(phase, message, self.gather_rows(phase, message))

    def stage0(k):
        n, j = k // per_matrix, k % per_matrix
        fresh = j < blocks
        q = (n + 1) * blocks + jnp.minimum(j, blocks - 1)

        @pl.when(fresh & (n + 1 < matrices))
        def _():
            load_a(q).wait()

            @pl.when(q - 1 + RAW < matrices * blocks)
            def _():
                load_a(q - 1 + RAW).start()

        load_g(k).wait()

        @pl.when(k + AHEAD < pieces)
        def _():
            load_g(k + AHEAD).start()

        p = Piece(k)
        slot = k % LEAVING

        def compute(turned, turned_next):
            turn(q, turned_next)
            acc[slot] = jnp.dot(turned[...], g_buf[k % (AHEAD + 1)], preferred_element_type=F32)

        @pl.when(n % 2 == 0)
        def _():
            compute(turned_even, turned_odd)

        @pl.when(n % 2 == 1)
        def _():
            compute(turned_odd, turned_even)

        far_out[p.leave, 0] = acc[slot, p.rows(0, 2), :].astype(BF16)
        far_out[p.leave, 1] = acc[slot, p.rows(0, -1), :].astype(BF16)
        p.reduce_copy(0, 0).start()
        p.reduce_copy(0, 1).start()

    def stage1(k):
        p = Piece(k)
        p.reduce_copy(0, 0).wait_recv()
        far_out[p.leave, 2] = (acc[k % LEAVING, p.rows(0, 1), :] + p.landed(0, 0)).astype(BF16)
        p.reduce_copy(0, 2).start()

    def stage2(k):
        p = Piece(k)
        p.reduce_copy(0, 1).wait_recv()
        p.reduce_copy(0, 2).wait_recv()
        slot = k % LEAVING
        half[slot] = acc[slot, p.rows(0, 0), :] + p.landed(0, 1) + p.landed(0, 2)
        near_out[p.leave, 0] = half[slot, p.rows(1, 2), :].astype(BF16)
        near_out[p.leave, 1] = half[slot, p.rows(1, -1), :].astype(BF16)
        p.reduce_copy(0, 0).wait_send()
        p.reduce_copy(0, 1).wait_send()
        p.reduce_copy(1, 0).start()
        p.reduce_copy(1, 1).start()

    def stage3(k):
        p = Piece(k)
        p.reduce_copy(1, 0).wait_recv()
        near_out[p.leave, 2] = (half[k % LEAVING, p.rows(1, 1), :] + p.landed(1, 0)).astype(BF16)
        p.reduce_copy(0, 2).wait_send()
        p.reduce_copy(1, 2).start()

    def stage4(k):
        p = Piece(k)
        p.reduce_copy(1, 1).wait_recv()
        p.reduce_copy(1, 2).wait_recv()
        out[k, p.own(0), :] = (half[k % LEAVING, p.rows(1, 0), :] + p.landed(1, 1) + p.landed(1, 2)).astype(BF16)
        p.reduce_copy(1, 0).wait_send()
        p.reduce_copy(1, 1).wait_send()
        p.gather(2, 0).start()
        p.gather(2, 1).start()

    def stage5(k):
        p = Piece(k)
        p.gather(2, 0).wait_recv()
        p.reduce_copy(1, 2).wait_send()
        p.gather(2, 2).start()

    def stage6(k):
        p = Piece(k)
        p.gather(2, 1).wait_recv()
        p.gather(2, 2).wait_recv()
        p.gather(2, 0).wait_send()
        p.gather(2, 1).wait_send()
        p.gather(3, 0).start()
        p.gather(3, 1).start()

    def stage7(k):
        p = Piece(k)
        p.gather(3, 0).wait_recv()
        p.gather(2, 2).wait_send()
        p.gather(3, 2).start()

    def stage8(k):
        p = Piece(k)
        p.gather(3, 1).wait_recv()
        p.gather(3, 2).wait_recv()
        p.gather(3, 0).wait_send()
        p.gather(3, 1).wait_send()

    def stage9(k):
        Piece(k).gather(3, 2).wait_send()

    stages = (stage0, stage1, stage2, stage3, stage4, stage5, stage6, stage7, stage8, stage9)

    @pl.loop(0, pieces + LAGS[-1])
    def _(i):
        for s in reversed(range(len(stages))):
            k = i - LAGS[s]

            @pl.when((k >= 0) & (k < pieces))
            def _(s=s, k=k):
                stages[s](k)


def place(held, out, sem):
    matrices, per_matrix = out.shape[0], out.shape[2] // WIDTH

    def move(k):
        columns = pl.ds(pl.multiple_of((k % per_matrix) * WIDTH, WIDTH), WIDTH)
        return pltpu.make_async_copy(held.at[k], out.at[k // per_matrix, :, columns], sem.at[k])

    for k in range(matrices * per_matrix):
        move(k).start()
    for k in range(matrices * per_matrix):
        move(k).wait()


def solution(mesh):
    side = math.isqrt(mesh.shape["dp"])

    def local(a, g):
        a, g = a[0], g[0]
        matrices, tokens, d = a.shape
        ff = g.shape[2]
        pieces = matrices * (ff // WIDTH)
        quarter = d // side
        part = quarter // side
        held = pl.pallas_call(
            functools.partial(kernel, side),
            out_shape=pltpu.VMEM((pieces, d, WIDTH), BF16),
            in_specs=[pl.BlockSpec(memory_space=pltpu.HBM)] * 2,
            out_specs=pl.BlockSpec(memory_space=pltpu.VMEM),
            scratch_shapes=[
                pltpu.VMEM((RAW, TURN, d), BF16),
                pltpu.VMEM((d, tokens), BF16),
                pltpu.VMEM((d, tokens), BF16),
                pltpu.VMEM((AHEAD + 1, tokens, WIDTH), BF16),
                pltpu.VMEM((LEAVING, d, WIDTH), F32),
                pltpu.VMEM((LEAVING, quarter, WIDTH), F32),
                pltpu.VMEM((LEAVING, 3, quarter, WIDTH), BF16),
                pltpu.VMEM((LEAVING, 3, part, WIDTH), BF16),
                pltpu.VMEM((LANDING, 3, quarter, WIDTH), BF16),
                pltpu.VMEM((LANDING, 3, part, WIDTH), BF16),
                pltpu.SemaphoreType.DMA((RAW,)),
                pltpu.SemaphoreType.DMA((AHEAD + 1,)),
                pltpu.SemaphoreType.DMA((4, 3, LEAVING)),
                pltpu.SemaphoreType.DMA((4, 3, LANDING)),
            ],
            compiler_params=pltpu.CompilerParams(
                collective_id=0, has_side_effects=True, vmem_limit_bytes=47 * 2**20
            ),
            cost_estimate=pl.CostEstimate(
                flops=2 * matrices * tokens * d * ff,
                bytes_accessed=2 * matrices * tokens * (d + ff),
                transcendentals=0,
            ),
            name="sum_over_group",
        )(a, g)
        return pl.pallas_call(
            place,
            out_shape=jax.ShapeDtypeStruct((matrices, d, ff), BF16),
            in_specs=[pl.BlockSpec(memory_space=pltpu.VMEM)],
            out_specs=pl.BlockSpec(memory_space=pltpu.HBM),
            scratch_shapes=[pltpu.SemaphoreType.DMA((pieces,))],
            compiler_params=pltpu.CompilerParams(vmem_limit_bytes=2**20),
            name="place",
        )(held)

    return jax.shard_map(
        local,
        mesh=mesh,
        in_specs=(P(("rep", "dp")), P(("rep", "dp"))),
        out_specs=P("rep"),
        check_vma=False,
    )
```

```python
import functools
import math

import jax
import jax.numpy as jnp
from jax import lax
from jax.experimental import pallas as pl
from jax.experimental.pallas import tpu as pltpu
from jax.sharding import PartitionSpec as P

MESH = pl.DeviceIdType.MESH
F32, BF16 = jnp.float32, jnp.bfloat16

WIDTH = 256
LAGS = (0, 3, 5, 8, 10, 12, 15, 18, 20, 22)
ORDER = (0, 1, 2, 3, 4, 5, 6, 7, 8, 9)
APART = tuple(later - sooner for sooner, later in zip(LAGS, LAGS[2:]))
LEAVING = max(APART) + 1
LANDING = 2 * LEAVING + 4
KEPT = max(APART[:4]) + 1
HELD = 2 * KEPT + 4
TURN = 512
RAW = 4
AHEAD = 2


def kernel(side, a_hbm, g_hbm, out, raw, turned_even, turned_odd, g_buf, acc, half, far_out, near_out, far_in, near_in, raw_sem, g_sem, send, recv):
    matrices, tokens, d = a_hbm.shape
    per_matrix = g_hbm.shape[2] // WIDTH
    pieces = matrices * per_matrix
    quarter = d // side
    part = quarter // side
    rep, me = lax.axis_index("rep"), lax.axis_index("dp")

    def step_from(axis, delta):
        stride = side * (1 - axis) + axis
        at = (me // stride) % side
        return me + ((at + delta + side) % side - at) * stride

    barrier = pltpu.get_barrier_semaphore()
    for axis in (0, 1):
        for delta in (1, -1):
            pl.semaphore_signal(barrier, inc=1, device_id=(rep, step_from(axis, delta)), device_id_type=MESH)

    blocks = tokens // TURN

    def load_a(q):
        at = pl.ds(pl.multiple_of((q % blocks) * TURN, TURN), TURN)
        return pltpu.make_async_copy(a_hbm.at[q // blocks, at, :], raw.at[q % RAW], raw_sem.at[q % RAW])

    def load_g(k):
        columns = pl.ds(pl.multiple_of((k % per_matrix) * WIDTH, WIDTH), WIDTH)
        slot = k % (AHEAD + 1)
        return pltpu.make_async_copy(g_hbm.at[k // per_matrix, :, columns], g_buf.at[slot], g_sem.at[slot])

    def turn(q, turned):
        at = pl.ds(pl.multiple_of((q % blocks) * TURN, TURN), TURN)
        turned[:, at] = raw[q % RAW].T

    for q in range(RAW):
        load_a(q).start()
    for k in range(AHEAD):
        load_g(k).start()

    @pl.loop(0, blocks)
    def _(q):
        load_a(q).wait()

        @pl.when(q > 0)
        def _():
            load_a(q - 1 + RAW).start()

        turn(q, turned_even)

    pl.semaphore_wait(barrier, 4)

    class Piece:
        def __init__(self, k):
            self.k = k
            self.axis = k % 2
            self.way = 1 - 2 * ((k // 2 + rep) % 2)
            stride = side * (1 - self.axis) + self.axis
            self.at = ((me // stride) % side, (me // (side + 1 - stride)) % side)
            self.land, self.leave = k % LANDING, k % LEAVING
            self.kept, self.held = k % KEPT, k % HELD

        def rows(self, phase, delta):
            size = (quarter, part)[phase]
            owner = (self.at[phase] + delta * self.way + 2 * side) % side
            return pl.ds(pl.multiple_of(owner * size, size), size)

        def own(self, delta):
            owner = (self.at[1] + delta * self.way + 2 * side) % side
            return pl.ds(pl.multiple_of(self.at[0] * quarter + owner * part, part), part)

        def copy(self, src, dst, phase, message):
            second = 1 if phase in (1, 2) else 0
            axis = self.axis * (1 - second) + (1 - self.axis) * second
            delta = self.way if message != 1 else -self.way
            return pltpu.make_async_remote_copy(
                src_ref=src,
                dst_ref=dst,
                send_sem=send.at[phase, message, self.leave],
                recv_sem=recv.at[phase, message, self.land],
                device_id=(rep, step_from(axis, delta)),
                device_id_type=MESH,
            )

        def reduce_copy(self, phase, message):
            leaving, landing = ((far_out, far_in), (near_out, near_in))[phase]
            return self.copy(leaving.at[self.kept, message], landing.at[self.held, message], phase, message)

        def landed(self, phase, message):
            return ((far_in, near_in)[phase])[self.held, message].astype(F32)

        def gather_copy(self, phase, message, rows):
            where = out.at[self.k, rows, :]
            return self.copy(where, where, phase, message)

        def gather_rows(self, phase, message):
            delta = 0 if message != 2 else -1
            return self.own(delta) if phase == 2 else self.rows(0, delta)

        def gather(self, phase, message):
            return self.gather_copy(phase, message, self.gather_rows(phase, message))

    def stage0(k):
        n, j = k // per_matrix, k % per_matrix
        fresh = j < blocks
        q = (n + 1) * blocks + jnp.minimum(j, blocks - 1)

        @pl.when(fresh & (n + 1 < matrices))
        def _():
            load_a(q).wait()

            @pl.when(q - 1 + RAW < matrices * blocks)
            def _():
                load_a(q - 1 + RAW).start()

        load_g(k).wait()

        @pl.when(k + AHEAD < pieces)
        def _():
            load_g(k + AHEAD).start()

        p = Piece(k)
        slot = k % KEPT

        def compute(turned, turned_next):
            turn(q, turned_next)
            acc[slot] = jnp.dot(turned[...], g_buf[k % (AHEAD + 1)], preferred_element_type=F32)

        @pl.when(n % 2 == 0)
        def _():
            compute(turned_even, turned_odd)

        @pl.when(n % 2 == 1)
        def _():
            compute(turned_odd, turned_even)

        far_out[p.kept, 0] = acc[slot, p.rows(0, 2), :].astype(BF16)
        far_out[p.kept, 1] = acc[slot, p.rows(0, -1), :].astype(BF16)
        p.reduce_copy(0, 0).start()
        p.reduce_copy(0, 1).start()

    def stage1(k):
        p = Piece(k)
        p.reduce_copy(0, 0).wait_recv()
        far_out[p.kept, 2] = (acc[k % KEPT, p.rows(0, 1), :] + p.landed(0, 0)).astype(BF16)
        p.reduce_copy(0, 2).start()

    def stage2(k):
        p = Piece(k)
        p.reduce_copy(0, 1).wait_recv()
        p.reduce_copy(0, 2).wait_recv()
        slot = k % KEPT
        half[slot] = acc[slot, p.rows(0, 0), :] + p.landed(0, 1) + p.landed(0, 2)
        near_out[p.kept, 0] = half[slot, p.rows(1, 2), :].astype(BF16)
        near_out[p.kept, 1] = half[slot, p.rows(1, -1), :].astype(BF16)
        p.reduce_copy(0, 0).wait_send()
        p.reduce_copy(0, 1).wait_send()
        p.reduce_copy(1, 0).start()
        p.reduce_copy(1, 1).start()

    def stage3(k):
        p = Piece(k)
        p.reduce_copy(1, 0).wait_recv()
        near_out[p.kept, 2] = (half[k % KEPT, p.rows(1, 1), :] + p.landed(1, 0)).astype(BF16)
        p.reduce_copy(0, 2).wait_send()
        p.reduce_copy(1, 2).start()

    def stage4(k):
        p = Piece(k)
        p.reduce_copy(1, 1).wait_recv()
        p.reduce_copy(1, 2).wait_recv()
        out[k, p.own(0), :] = (half[k % KEPT, p.rows(1, 0), :] + p.landed(1, 1) + p.landed(1, 2)).astype(BF16)
        p.reduce_copy(1, 0).wait_send()
        p.reduce_copy(1, 1).wait_send()
        p.gather(2, 0).start()
        p.gather(2, 1).start()

    def stage5(k):
        p = Piece(k)
        p.gather(2, 0).wait_recv()
        p.reduce_copy(1, 2).wait_send()
        p.gather(2, 2).start()

    def stage6(k):
        p = Piece(k)
        p.gather(2, 1).wait_recv()
        p.gather(2, 2).wait_recv()
        p.gather(2, 0).wait_send()
        p.gather(2, 1).wait_send()
        p.gather(3, 0).start()
        p.gather(3, 1).start()

    def stage7(k):
        p = Piece(k)
        p.gather(3, 0).wait_recv()
        p.gather(2, 2).wait_send()
        p.gather(3, 2).start()

    def stage8(k):
        p = Piece(k)
        p.gather(3, 1).wait_recv()
        p.gather(3, 2).wait_recv()
        p.gather(3, 0).wait_send()
        p.gather(3, 1).wait_send()

    def stage9(k):
        Piece(k).gather(3, 2).wait_send()

    stages = (stage0, stage1, stage2, stage3, stage4, stage5, stage6, stage7, stage8, stage9)

    @pl.loop(0, pieces + LAGS[-1])
    def _(i):
        for s in ORDER:
            k = i - LAGS[s]

            @pl.when((k >= 0) & (k < pieces))
            def _(s=s, k=k):
                stages[s](k)


def place(held, out, sem):
    matrices, per_matrix = out.shape[0], out.shape[2] // WIDTH

    def move(k):
        columns = pl.ds(pl.multiple_of((k % per_matrix) * WIDTH, WIDTH), WIDTH)
        return pltpu.make_async_copy(held.at[k], out.at[k // per_matrix, :, columns], sem.at[k])

    for k in range(matrices * per_matrix):
        move(k).start()
    for k in range(matrices * per_matrix):
        move(k).wait()


def solution(mesh):
    side = math.isqrt(mesh.shape["dp"])

    def local(a, g):
        a, g = a[0], g[0]
        matrices, tokens, d = a.shape
        ff = g.shape[2]
        pieces = matrices * (ff // WIDTH)
        quarter = d // side
        part = quarter // side
        held = pl.pallas_call(
            functools.partial(kernel, side),
            out_shape=pltpu.VMEM((pieces, d, WIDTH), BF16),
            in_specs=[pl.BlockSpec(memory_space=pltpu.HBM)] * 2,
            out_specs=pl.BlockSpec(memory_space=pltpu.VMEM),
            scratch_shapes=[
                pltpu.VMEM((RAW, TURN, d), BF16),
                pltpu.VMEM((d, tokens), BF16),
                pltpu.VMEM((d, tokens), BF16),
                pltpu.VMEM((AHEAD + 1, tokens, WIDTH), BF16),
                pltpu.VMEM((KEPT, d, WIDTH), F32),
                pltpu.VMEM((KEPT, quarter, WIDTH), F32),
                pltpu.VMEM((KEPT, 3, quarter, WIDTH), BF16),
                pltpu.VMEM((KEPT, 3, part, WIDTH), BF16),
                pltpu.VMEM((HELD, 3, quarter, WIDTH), BF16),
                pltpu.VMEM((HELD, 3, part, WIDTH), BF16),
                pltpu.SemaphoreType.DMA((RAW,)),
                pltpu.SemaphoreType.DMA((AHEAD + 1,)),
                pltpu.SemaphoreType.DMA((4, 3, LEAVING)),
                pltpu.SemaphoreType.DMA((4, 3, LANDING)),
            ],
            compiler_params=pltpu.CompilerParams(
                collective_id=0, has_side_effects=True, vmem_limit_bytes=47 * 2**20
            ),
            cost_estimate=pl.CostEstimate(
                flops=2 * matrices * tokens * d * ff,
                bytes_accessed=2 * matrices * tokens * (d + ff),
                transcendentals=0,
            ),
            name="sum_over_group",
        )(a, g)
        return pl.pallas_call(
            place,
            out_shape=jax.ShapeDtypeStruct((matrices, d, ff), BF16),
            in_specs=[pl.BlockSpec(memory_space=pltpu.VMEM)],
            out_specs=pl.BlockSpec(memory_space=pltpu.HBM),
            scratch_shapes=[pltpu.SemaphoreType.DMA((pieces,))],
            compiler_params=pltpu.CompilerParams(vmem_limit_bytes=2**20),
            name="place",
        )(held)

    return jax.shard_map(
        local,
        mesh=mesh,
        in_specs=(P(("rep", "dp")), P(("rep", "dp"))),
        out_specs=P("rep"),
        check_vma=False,
    )
```
